16 devices in a mesh: dp: 2 (over y, z), dpa: 8 (over x, core).
Axes of the slice: x: 4, y: 2, z: 1, core: 2. Of those that a mesh axis runs over, the one named last changes fastest.
The devices are a block of a 4x4x8 slice.
Arguments:
- x: bfloat16 [16, 4, 512, 2048], P(('dp', 'dpa')), parts along dimension 0
- chunk_len: int32 [16, 4], P(('dp', 'dpa')), parts along dimension 0
- ctx_len: int32 [16, 4], P(('dp', 'dpa')), parts along dimension 0
- lat_cache: bfloat16 [16, 4, 1024, 512], P(('dp', 'dpa')), parts along dimension 0
- rope_cache: bfloat16 [16, 4, 1024, 64], P(('dp', 'dpa')), parts along dimension 0
- topk_idx: int32 [16, 4, 512, 6], P(('dp', 'dpa')), parts along dimension 0
- g_attn: bfloat16 [2048], replicated
- w_q: bfloat16 [2048, 16, 192], replicated
- w_dkv: bfloat16 [2048, 512], replicated
- g_kv: bfloat16 [512], replicated
- w_kr: bfloat16 [2048, 64], replicated
- w_uk: bfloat16 [512, 16, 128], replicated
- w_uv: bfloat16 [512, 16, 128], replicated
- w_o: bfloat16 [16, 128, 2048], replicated
- g_ffn: bfloat16 [2048], replicated
- w_router: bfloat16 [2048, 64], replicated
- w_sh_gate: bfloat16 [2048, 2816], replicated
- w_sh_up: bfloat16 [2048, 2816], replicated
- w_sh_down: bfloat16 [2816, 2048], replicated
- w_exp_gate: bfloat16 [64, 2048, 1408], P('dpa')
- w_exp_up: bfloat16 [64, 2048, 1408], P('dpa')
- w_exp_down: bfloat16 [64, 1408, 2048], P('dpa')
Outputs:
- output 1: bfloat16 [16, 4, 512, 2048], P(('dp', 'dpa')), parts along dimension 0
- output 2: bfloat16 [16, 4, 1024, 512], P(('dp', 'dpa')), parts along dimension 0
- output 3: bfloat16 [16, 4, 1024, 64], P(('dp', 'dpa')), parts along dimension 0
There are 2 independent parts. The reference program is written for one: setup_inputs(seed, part) draws one part's arguments, and reference() takes and returns one part's arrays. A program takes and returns all parts, laid end to end along the dimension named above; an argument that names none is the same for every part.
All inputs are finite; a program needn't handle non-finite values.
Results may differ from the reference program's by a relative error of at most 0.0196382.
Values are sent between devices in bfloat16 or wider.
A program may use at most 768 MiB of HBM per device.

```python
import jax
import jax.numpy as jnp
from jax import lax

GROUP = 8
REQS = 4
CHUNK = 512
CTX = 1024
HID = 2048
HEADS = 16
NOPE = 128
ROPE = 64
VDIM = 128
RANK = 512
EXPERTS = 64
EXP_FF = 1408
SHARED_FF = 2816
TOP = 6
BLOCK_ROWS = 128

TOKENS = REQS * CHUNK
LOCAL = EXPERTS // GROUP
QDIM = NOPE + ROPE
EPS = 1e-6
THETA = 10000.0


def draw_normal(rand_key, shape, scale):
    return (jax.random.normal(rand_key, shape, jnp.float32) * scale).astype(jnp.bfloat16)


def draw_gain(rand_key, width):
    return jax.random.uniform(rand_key, (width,), jnp.float32, 0.5, 1.5).astype(jnp.bfloat16)


def draw_lengths(rand_key):
    chunk_key, ctx_key = jax.random.split(rand_key)
    chunk_len = jax.random.randint(chunk_key, (GROUP, REQS), CHUNK // 4, CHUNK + 1).astype(jnp.int32)
    ctx_len = jax.random.randint(ctx_key, (GROUP, REQS), CTX // 8, CTX - CHUNK + 1).astype(jnp.int32)
    return chunk_len.at[0, 0].set(CHUNK), ctx_len.at[GROUP - 1, REQS - 1].set(CTX - CHUNK)


def draw_routes(rand_key):
    start_key, local_key = jax.random.split(rand_key)
    shuffled = jax.vmap(lambda sub_key: jax.random.permutation(sub_key, TOKENS))(jax.random.split(start_key, GROUP))
    first_dev = shuffled % GROUP
    first_loc = jax.random.randint(local_key, (GROUP, TOKENS), 0, LOCAL)
    slot_ids = jnp.arange(TOP)
    target = (first_dev[:, :, None] + slot_ids) % GROUP
    local_id = (first_loc[:, :, None] + slot_ids // GROUP) % LOCAL
    return (target * LOCAL + local_id).reshape(GROUP, REQS, CHUNK, TOP).astype(jnp.int32)


def setup_inputs(seed: int = 0, part: int = 0) -> dict:
    base_key = jax.random.key(seed)
    part_keys = jax.random.split(jax.random.fold_in(base_key, part), 6)
    shared_keys = jax.random.split(base_key, 16)
    chunk_len, ctx_len = draw_lengths(part_keys[0])
    return {
        'x': draw_normal(part_keys[1], (GROUP, REQS, CHUNK, HID), 1.0),
        'chunk_len': chunk_len,
        'ctx_len': ctx_len,
        'lat_cache': draw_normal(part_keys[2], (GROUP, REQS, CTX, RANK), 1.0),
        'rope_cache': draw_normal(part_keys[3], (GROUP, REQS, CTX, ROPE), 1.0),
        'topk_idx': draw_routes(part_keys[4]),
        'g_attn': draw_gain(shared_keys[0], HID),
        'w_q': draw_normal(shared_keys[1], (HID, HEADS, QDIM), HID ** -0.5),
        'w_dkv': draw_normal(shared_keys[2], (HID, RANK), HID ** -0.5),
        'g_kv': draw_gain(shared_keys[3], RANK),
        'w_kr': draw_normal(shared_keys[4], (HID, ROPE), HID ** -0.5),
        'w_uk': draw_normal(shared_keys[5], (RANK, HEADS, NOPE), 2.5 * NOPE ** -0.5),
        'w_uv': draw_normal(shared_keys[6], (RANK, HEADS, VDIM), RANK ** -0.5),
        'w_o': draw_normal(shared_keys[7], (HEADS, VDIM, HID), 4.0 * (HEADS * VDIM) ** -0.5),
        'g_ffn': draw_gain(shared_keys[8], HID),
        'w_router': draw_normal(shared_keys[9], (HID, EXPERTS), HID ** -0.5),
        'w_sh_gate': draw_normal(shared_keys[10], (HID, SHARED_FF), HID ** -0.5),
        'w_sh_up': draw_normal(shared_keys[11], (HID, SHARED_FF), HID ** -0.5),
        'w_sh_down': draw_normal(shared_keys[12], (SHARED_FF, HID), SHARED_FF ** -0.5),
        'w_exp_gate': draw_normal(shared_keys[13], (EXPERTS, HID, EXP_FF), HID ** -0.5),
        'w_exp_up': draw_normal(shared_keys[14], (EXPERTS, HID, EXP_FF), HID ** -0.5),
        'w_exp_down': draw_normal(shared_keys[15], (EXPERTS, EXP_FF, HID), 0.8 * EXPERTS * EXP_FF ** -0.5),
    }


def rms_norm(vals, gain):
    vals_f32 = vals.astype(jnp.float32)
    inv_rms = lax.rsqrt(jnp.mean(vals_f32 * vals_f32, axis=-1, keepdims=True) + EPS)
    return (vals_f32 * inv_rms * gain.astype(jnp.float32)).astype(jnp.bfloat16)


def rope_tables(positions):
    inv_freq = THETA ** (-2.0 * jnp.arange(ROPE // 2, dtype=jnp.float32) / ROPE)
    angle = positions.astype(jnp.float32)[..., None] * inv_freq
    return jnp.cos(angle), jnp.sin(angle)


def rotate(vals, cos_tab, sin_tab):
    half = ROPE // 2
    first = vals[..., :half]
    second = vals[..., half:]
    return jnp.concatenate([first * cos_tab - second * sin_tab, second * cos_tab + first * sin_tab], axis=-1)


def write_window(cache_row, new_rows, start, keep):
    old_rows = lax.dynamic_slice_in_dim(cache_row, start, CHUNK, axis=0)
    merged = jnp.where(keep[:, None], new_rows, old_rows)
    return lax.dynamic_update_slice_in_dim(cache_row, merged, start, axis=0)


def reference(x, chunk_len, ctx_len, lat_cache, rope_cache, topk_idx, g_attn, w_q, w_dkv, g_kv, w_kr, w_uk, w_uv, w_o, g_ffn, w_router, w_sh_gate, w_sh_up, w_sh_down, w_exp_gate, w_exp_up, w_exp_down):
    def one_request(args):
        x_req, req_chunk, req_ctx, lat_old, rope_old = args
        normed = rms_norm(x_req, g_attn)
        q_full = jnp.dot(normed, w_q.reshape(HID, HEADS * QDIM), preferred_element_type=jnp.float32).astype(jnp.bfloat16).reshape(CHUNK, HEADS, QDIM)
        positions = req_ctx + jnp.arange(CHUNK)
        cos_tab, sin_tab = rope_tables(positions)
        q_rope = rotate(q_full[:, :, NOPE:].astype(jnp.float32), cos_tab[:, None, :], sin_tab[:, None, :]).astype(jnp.bfloat16)
        q_lat = jnp.einsum('chn,khn->chk', q_full[:, :, :NOPE].astype(jnp.float32), w_uk.astype(jnp.float32)).astype(jnp.bfloat16)
        lat_new = rms_norm(jnp.dot(normed, w_dkv, preferred_element_type=jnp.float32), g_kv)
        rope_new = rotate(jnp.dot(normed, w_kr, preferred_element_type=jnp.float32), cos_tab, sin_tab).astype(jnp.bfloat16)
        keep = jnp.arange(CHUNK) < req_chunk
        lat_upd = write_window(lat_old, lat_new, req_ctx, keep)
        rope_upd = write_window(rope_old, rope_new, req_ctx, keep)
        lat_f32 = lat_upd.astype(jnp.float32)
        scores = (jnp.einsum('chk,lk->chl', q_lat.astype(jnp.float32), lat_f32) + jnp.einsum('chp,lp->chl', q_rope.astype(jnp.float32), rope_upd.astype(jnp.float32))) * QDIM ** -0.5
        visible = jnp.arange(CTX)[None, None, :] <= positions[:, None, None]
        scores = jnp.where(visible, scores, -1e30)
        attn_prob = jax.nn.softmax(scores, axis=-1).astype(jnp.bfloat16)
        out_lat = jnp.einsum('chl,lk->chk', attn_prob.astype(jnp.float32), lat_f32).astype(jnp.bfloat16)
        out_head = jnp.einsum('chk,khv->chv', out_lat.astype(jnp.float32), w_uv.astype(jnp.float32)).astype(jnp.bfloat16)
        attn_out = jnp.dot(out_head.reshape(CHUNK, HEADS * VDIM), w_o.reshape(HEADS * VDIM, HID), preferred_element_type=jnp.float32).astype(jnp.bfloat16)
        hidden = (x_req.astype(jnp.float32) + attn_out.astype(jnp.float32)).astype(jnp.bfloat16)
        return hidden, lat_upd, rope_upd

    reqs_all = GROUP * REQS
    hidden, lat_upd, rope_upd = lax.map(one_request, (x.reshape(reqs_all, CHUNK, HID), chunk_len.reshape(reqs_all), ctx_len.reshape(reqs_all), lat_cache.reshape(reqs_all, CTX, RANK), rope_cache.reshape(reqs_all, CTX, ROPE)))
    rows = GROUP * TOKENS
    pairs = rows * TOP
    flat_h = hidden.reshape(rows, HID)
    normed = rms_norm(flat_h, g_ffn)
    valid = (jnp.arange(CHUNK)[None, :] < chunk_len.reshape(reqs_all, 1)).reshape(rows)
    route_prob = jax.nn.softmax(jnp.dot(normed, w_router, preferred_element_type=jnp.float32), axis=-1)
    choice = topk_idx.reshape(rows, TOP)
    gates = jnp.take_along_axis(route_prob, choice, axis=1)
    shared_act = (jax.nn.silu(jnp.dot(normed, w_sh_gate, preferred_element_type=jnp.float32)) * jnp.dot(normed, w_sh_up, preferred_element_type=jnp.float32)).astype(jnp.bfloat16)
    shared_out = jnp.dot(shared_act, w_sh_down, preferred_element_type=jnp.float32)
    pair_ok = jnp.repeat(valid, TOP)
    pair_key = jnp.where(pair_ok, choice.reshape(pairs), EXPERTS)
    counts = jnp.bincount(pair_key, length=EXPERTS + 1)
    padded = (counts[:EXPERTS] + BLOCK_ROWS - 1) // BLOCK_ROWS * BLOCK_ROWS
    pad_start = jnp.cumsum(padded) - padded
    raw_start = jnp.cumsum(counts) - counts
    order = jnp.argsort(pair_key, stable=True)
    sorted_key = pair_key[order]
    num_blocks = pairs // BLOCK_ROWS + EXPERTS + 1
    slots = num_blocks * BLOCK_ROWS
    start_ext = jnp.concatenate([pad_start, jnp.full((1,), slots, pad_start.dtype)])
    slot_of_sorted = start_ext[sorted_key] + jnp.arange(pairs) - raw_start[sorted_key]
    slot_pair = jnp.full((slots,), pairs, order.dtype).at[slot_of_sorted].set(order, mode='drop')
    slot_token = slot_pair // TOP
    gate_ext = jnp.concatenate([gates.reshape(pairs), jnp.zeros((1,), jnp.float32)])
    slot_gate = gate_ext[slot_pair]
    block_start = jnp.arange(num_blocks) * BLOCK_ROWS
    block_exp = jnp.clip(jnp.sum(pad_start[None, :] <= block_start[:, None], axis=1) - 1, 0, EXPERTS - 1)
    normed_ext = jnp.concatenate([normed, jnp.zeros((1, HID), jnp.bfloat16)])

    def expert_block(routed, args):
        tok_ids, tok_gate, exp_id = args
        block_in = normed_ext[tok_ids].astype(jnp.float32)
        gate_w = lax.dynamic_index_in_dim(w_exp_gate, exp_id, 0, keepdims=False).astype(jnp.float32)
        up_w = lax.dynamic_index_in_dim(w_exp_up, exp_id, 0, keepdims=False).astype(jnp.float32)
        down_w = lax.dynamic_index_in_dim(w_exp_down, exp_id, 0, keepdims=False).astype(jnp.float32)
        act = (jax.nn.silu(jnp.dot(block_in, gate_w)) * jnp.dot(block_in, up_w)).astype(jnp.bfloat16)
        block_out = jnp.dot(act.astype(jnp.float32), down_w).astype(jnp.bfloat16)
        routed = routed.at[tok_ids].add(tok_gate[:, None] * block_out.astype(jnp.float32), mode='drop')
        return routed, tok_ids[0]

    routed = lax.scan(expert_block, jnp.zeros((rows, HID), jnp.float32), (slot_token.reshape(num_blocks, BLOCK_ROWS), slot_gate.reshape(num_blocks, BLOCK_ROWS), block_exp))[0]
    total = flat_h.astype(jnp.float32) + shared_out + routed
    result = jnp.where(valid[:, None], total, 0.0).astype(jnp.bfloat16).reshape(GROUP, REQS, CHUNK, HID)
    return result, lat_upd.reshape(GROUP, REQS, CTX, RANK), rope_upd.reshape(GROUP, REQS, CTX, ROPE)
```

```python
import functools

import jax
import jax.numpy as jnp
from jax import lax
from jax.experimental import pallas as pl
from jax.experimental.pallas import tpu as pltpu
from jax.sharding import PartitionSpec as P

EPS = 1e-6
THETA = 10000.0
NEG = -1e30
UNIT = 16
PIECE = 256
KBLK = 256
TBLK = 128
VMEM = pltpu.VMEM
SMEM = pltpu.SMEM
ANY = pl.ANY
F32 = jnp.float32
BF16 = jnp.bfloat16


def rms_norm(vals, gain):
    vals_f32 = vals.astype(F32)
    inv_rms = lax.rsqrt(jnp.mean(vals_f32 * vals_f32, axis=-1, keepdims=True) + EPS)
    return (vals_f32 * inv_rms * gain.astype(F32)).astype(BF16)


def dot(lhs, rhs):
    return jnp.dot(lhs, rhs, preferred_element_type=F32)


def whole_spec(shape):
    return pl.BlockSpec(shape, lambda *_: (0,) * len(shape), pipeline_mode=pl.Buffered(1))


def attention_kernel(lens, x_ref, a_ref, q_ref, wuk_ref, wuv_ref, wdkv_ref, wkr_ref, cos_ref, sin_ref, perm_ref, gkv_ref, gffn_ref, wo_ref, lat_ref, rope_ref, h_ref, u_ref, lat_out, rope_out, keys_ref, o_ref, *, heads_step, row_blk, key_blk, scale, nope, rope):
    step = pl.program_id(0)
    count, ctx = lens[0], lens[1]
    chunk, width = x_ref.shape
    rank = lat_ref.shape[1]
    ctx_max = lat_ref.shape[0]

    @pl.when(step == 0)
    def _():
        a_val = a_ref[...]
        lat_f32 = dot(a_val, wdkv_ref[...])
        inv_rms = lax.rsqrt(jnp.mean(lat_f32 * lat_f32, axis=-1, keepdims=True) + EPS)
        lat_new = (lat_f32 * inv_rms * gkv_ref[...].astype(F32)).astype(BF16)
        both = dot(a_val, wkr_ref[...])
        rope_new = (both[:, :rope] * cos_ref[...] + both[:, rope:] * sin_ref[...]).astype(BF16)
        for base in range(0, ctx_max, key_blk):
            pos = lax.broadcasted_iota(jnp.int32, (key_blk, chunk), 0) + base - ctx
            row = lax.broadcasted_iota(jnp.int32, (key_blk, chunk), 1)
            pick = ((pos == row) & (row < count)).astype(F32).astype(BF16)
            at = lax.broadcasted_iota(jnp.int32, (key_blk, 1), 0) + base - ctx
            fresh = (at >= 0) & (at < count)
            rows = pl.ds(base, key_blk)
            lat_blk = jnp.where(fresh, dot(pick, lat_new), lat_ref[rows, :].astype(F32))
            rope_blk = jnp.where(fresh, dot(pick, rope_new), rope_ref[rows, :].astype(F32))
            lat_out[rows, :] = lat_blk.astype(BF16)
            rope_out[rows, :] = rope_blk.astype(BF16)
            keys_ref[0:rank, base:base + key_blk] = lat_blk.T.astype(BF16)
            keys_ref[rank:rank + rope, base:base + key_blk] = rope_blk.T.astype(BF16)

    vdim = wuv_ref.shape[2]
    for row0 in range(0, chunk, row_blk):
        rows = slice(row0, row0 + row_blk)
        seen = ctx + jnp.minimum(count, row0 + row_blk)
        blocks = (seen + key_blk - 1) // key_blk
        for n_keys in range(1, ctx_max // key_blk + 1):
            @pl.when((row0 < count) & (blocks == n_keys))
            def _():
                span = n_keys * key_blk
                col = lax.broadcasted_iota(jnp.int32, (row_blk, span), 1)
                row = lax.broadcasted_iota(jnp.int32, (row_blk, span), 0)
                visible = col - row <= ctx + row0
                for sub in range(heads_step):
                    q_val = q_ref[sub, rows, :]
                    q_lat = dot(q_val[:, :nope], wuk_ref[sub]).astype(BF16)
                    q_raw = q_val[:, nope:nope + rope]
                    q_rot = (q_raw.astype(F32) * cos_ref[rows, :] + dot(q_raw, perm_ref[...]) * sin_ref[rows, :]).astype(BF16)
                    scores = (dot(q_lat, keys_ref[0:rank, :span]) + dot(q_rot, keys_ref[rank:rank + rope, :span])) * scale
                    scores = jnp.where(visible, scores, NEG)
                    top = jnp.max(scores, axis=1, keepdims=True)
                    expo = jnp.exp(scores - top)
                    prob = (expo * (1.0 / jnp.sum(expo, axis=1, keepdims=True))).astype(BF16)
                    out_lat = dot(prob, lat_out[0:span, :]).astype(BF16)
                    head = step * heads_step + sub
                    o_ref[rows, pl.ds(pl.multiple_of(head * vdim, vdim), vdim)] = dot(out_lat, wuv_ref[sub]).astype(BF16)

    @pl.when(step == pl.num_programs(0) - 1)
    def _():
        for row0 in range(0, chunk, row_blk):
            rows = slice(row0, row0 + row_blk)

            @pl.when(row0 < count)
            def _():
                def column(index, carry):
                    cols = pl.ds(pl.multiple_of(index * 512, 512), 512)
                    attn = dot(o_ref[rows, :], wo_ref[:, cols]).astype(BF16)
                    h_ref[rows, cols] = (x_ref[rows, cols].astype(F32) + attn.astype(F32)).astype(BF16)
                    return carry

                lax.fori_loop(0, width // 512, column, 0)
                u_ref[rows, :] = rms_norm(h_ref[rows, :], gffn_ref[...])

            @pl.when(row0 >= count)
            def _():
                h_ref[rows, :] = jnp.zeros((row_blk, width), BF16)
                u_ref[rows, :] = jnp.zeros((row_blk, width), BF16)


def attention(req, lens, x_all, a_req, q_req, wuk, wuv, wdkv, wkr2, cos_tab, sin_tab, perm, gkv, gffn, wo, lat_all, rope_all):
    n_req, chunk, width = x_all.shape
    heads, _, qdim = q_req.shape
    rope = perm.shape[0]
    nope = qdim - rope
    _, ctx_max, rank = lat_all.shape
    vdim = wuv.shape[2]
    hstep = 2
    kernel = functools.partial(attention_kernel, heads_step=hstep, row_blk=256, key_blk=256, scale=qdim ** -0.5, nope=nope, rope=rope)

    def one(shape):
        return pl.BlockSpec((None,) + shape, lambda *_: (req,) + (0,) * len(shape), pipeline_mode=pl.Buffered(1))

    def per_head(shape):
        return pl.BlockSpec((hstep,) + shape, lambda i, *_: (i, 0, 0))

    return pl.pallas_call(
        kernel,
        grid_spec=pltpu.PrefetchScalarGridSpec(
            num_scalar_prefetch=1,
            grid=(heads // hstep,),
            in_specs=[
                one((chunk, width)),
                whole_spec((chunk, width)),
                per_head((chunk, qdim)),
                per_head((nope, rank)),
                per_head((rank, vdim)),
                whole_spec(wdkv.shape),
                whole_spec(wkr2.shape),
                one((chunk, rope)),
                one((chunk, rope)),
                whole_spec(perm.shape),
                whole_spec(gkv.shape),
                whole_spec(gffn.shape),
                whole_spec(wo.shape),
                one((ctx_max, rank)),
                one((ctx_max, rope)),
            ],
            out_specs=[
                whole_spec((chunk, width)),
                whole_spec((chunk, width)),
                one((ctx_max, rank)),
                one((ctx_max, rope)),
            ],
            scratch_shapes=[VMEM((rank + rope, ctx_max), BF16), VMEM((chunk, heads * vdim), BF16)],
        ),
        out_shape=[
            jax.ShapeDtypeStruct((chunk, width), BF16),
            jax.ShapeDtypeStruct((chunk, width), BF16),
            jax.ShapeDtypeStruct(lat_all.shape, BF16),
            jax.ShapeDtypeStruct(rope_all.shape, BF16),
        ],
        input_output_aliases={14: 2, 15: 3},
        compiler_params=pltpu.CompilerParams(vmem_limit_bytes=58 << 20),
        cost_estimate=pl.CostEstimate(flops=30 * 10 ** 9, bytes_accessed=24 << 20, transcendentals=chunk * heads * ctx_max // 2),
        name=f"attention_{req}",
    )(lens, x_all, a_req, q_req, wuk, wuv, wdkv, wkr2, cos_tab, sin_tab, perm, gkv, gffn, wo, lat_all, rope_all)


def slot_table(topk, valid, n_exp, group):
    tokens, top_k = topk.shape
    local = n_exp // group
    ids = jnp.arange(n_exp, dtype=jnp.int32)
    hit = jnp.any(topk.T[:, None, :] == ids[None, :, None], axis=0) & valid[None, :]
    incl = jnp.cumsum(hit.astype(jnp.int32), axis=1)
    before = incl - hit.astype(jnp.int32)
    units = (incl[:, -1] + UNIT - 1) // UNIT
    turn = (before // UNIT).reshape(group, local, tokens)
    rank = jnp.zeros_like(turn)
    own = jnp.arange(local, dtype=jnp.int32)[None, :, None]
    per = units.reshape(group, local)
    for other in range(local):
        have = per[:, other][:, None, None]
        rank = rank + jnp.minimum(have, turn) + ((own > other) & (have > turn)).astype(jnp.int32)
    slot = rank.reshape(n_exp, tokens) * UNIT + before % UNIT
    return jnp.where(hit, slot, -1), jnp.sum(per, axis=1)


def owner_tables(slots, n_pieces):
    group, local, tokens = slots.shape
    per = PIECE // UNIT
    units = (jnp.sum((slots >= 0).astype(jnp.int32), axis=2) + UNIT - 1) // UNIT
    cap = n_pieces * per
    turn = jnp.arange(tokens // UNIT, dtype=jnp.int32)[None, None, :]
    rank = jnp.zeros((group, local, tokens // UNIT), jnp.int32)
    own = jnp.arange(local, dtype=jnp.int32)[None, :, None]
    for other in range(local):
        have = units[:, other][:, None, None]
        rank = rank + jnp.minimum(have, turn) + ((own > other) & (have > turn)).astype(jnp.int32)
    rank = jnp.where(turn < units[:, :, None], rank, -1)
    expert = jnp.max(jnp.where(rank[:, None, :, :] == jnp.arange(cap, dtype=jnp.int32)[None, :, None, None], own[:, None], -1), axis=(2, 3))
    expert = jnp.where(expert < 0, local, expert).reshape(group, n_pieces, per).transpose(1, 0, 2).reshape(n_pieces, group * per)
    order = jnp.arange(group * per, dtype=jnp.int32)
    key = expert * (group * per) + order
    pos = jnp.sum((key[:, None, :] < key[:, :, None]).astype(jnp.int32), axis=2)
    inv = jnp.sum(jnp.where(pos[:, None, :] == order[None, :, None], order[None, None, :], 0), axis=2)
    first = jnp.sum((expert[:, None, :] < jnp.arange(local + 1, dtype=jnp.int32)[None, :, None]).astype(jnp.int32), axis=2)
    n_blk = tokens // KBLK
    piece = jnp.where(slots >= 0, slots // PIECE, -1).reshape(group, local, n_blk, KBLK)
    active = jnp.any(piece[None] == jnp.arange(n_pieces, dtype=jnp.int32)[:, None, None, None, None], axis=(2, 4)).reshape(n_pieces, group * n_blk)
    items, n_items = compact(active)
    return pos, inv, first, items, n_items


def compact(active):
    size = active.shape[-1]
    ids = jnp.arange(size, dtype=jnp.int32)
    flag = active.astype(jnp.int32)
    place = jnp.sum(jnp.where(ids[None, :] < ids[:, None], flag[:, None, :], 0), axis=2)
    items = jnp.sum(jnp.where((place[:, None, :] == ids[None, :, None]) & active[:, None, :], ids[None, None, :], 0), axis=2)
    return items, jnp.sum(flag, axis=1)


def expert_kernel(n_src, pos_ref, inv_ref, first_ref, item_ref, count_ref, slot_ref, *refs, n_req, piece):
    u_refs = refs[:n_req]
    wg_hbm, wu_hbm, wd_hbm, out_hbm, trash, wgu, wdn, rows_ref, acc, ubuf, obuf, zbuf, wsem, usem, osem, zsem = refs[n_req:]
    local = wg_hbm.shape[0]
    ff = wg_hbm.shape[2]
    per = piece // UNIT
    tile = obuf.shape[1]
    tile_units = tile // UNIT
    n_blk = slot_ref.shape[1] // KBLK
    req_blk = n_blk // n_req
    n_items = count_ref[0]
    depth = ubuf.shape[0]
    base = count_ref[1]

    def weights(exp, slot):
        return (
            pltpu.make_async_copy(wg_hbm.at[exp], wgu.at[slot, :, pl.ds(0, ff)], wsem.at[slot, 0]),
            pltpu.make_async_copy(wu_hbm.at[exp], wgu.at[slot, :, pl.ds(ff, ff)], wsem.at[slot, 1]),
            pltpu.make_async_copy(wd_hbm.at[exp], wdn.at[slot], wsem.at[slot, 2]),
        )

    def token_copy(ref, src, blk, slot):
        start = pl.multiple_of((src * req_blk + blk % req_blk) * KBLK, KBLK)
        return pltpu.make_async_copy(ref.at[pl.ds(start, KBLK), :], ubuf.at[slot], usem.at[slot])

    def fetch(index):
        item = item_ref[index]
        src, blk = item // n_blk, item % n_blk
        for req in range(n_req):
            @pl.when(blk // req_blk == req)
            def _():
                token_copy(u_refs[req], src, blk, index % depth).start()

    @pl.when(n_items > 0)
    def _():
        for copy in weights(0, 0):
            copy.start()
        for index in range(depth - 1):
            @pl.when(index < n_items)
            def _():
                fetch(index)

    zbuf[...] = jnp.zeros_like(zbuf)
    used = first_ref[local]

    def unit_rows(unit):
        return pl.ds(pl.multiple_of(unit * UNIT, UNIT), UNIT)

    def blank(index, carry):
        pltpu.make_async_copy(zbuf, out_hbm.at[unit_rows(inv_ref[index])], zsem).start()
        return carry

    lax.fori_loop(used, n_src * per, blank, 0)

    def gather(index, carry):
        item = item_ref[index]
        src, blk = item // n_blk, item % n_blk
        slot = index % depth
        token_copy(u_refs[0], 0, 0, slot).wait()

        @pl.when(index + depth - 1 < n_items)
        def _():
            fetch(index + depth - 1)

        at = slot_ref[pl.ds(pl.multiple_of(src * local, local), local), pl.ds(pl.multiple_of(blk * KBLK, KBLK), KBLK)] - base
        row = lax.broadcasted_iota(jnp.int32, (piece, KBLK), 0)
        pick = at[0:1, :] == row
        for exp in range(1, local):
            pick = pick | (at[exp:exp + 1, :] == row)
        part = dot(pick.astype(F32).astype(BF16), ubuf[slot])
        prev = item_ref[jnp.maximum(index - 1, 0)] // n_blk
        after = item_ref[jnp.minimum(index + 1, n_items - 1)] // n_blk
        opens = (index == 0) | (prev != src)
        closes = (index == n_items - 1) | (after != src)

        @pl.when(opens)
        def _():
            acc[...] = part

        @pl.when(jnp.logical_not(opens))
        def _():
            acc[...] += part

        @pl.when(closes)
        def _():
            for unit in range(per):
                rows_ref[unit_rows(pos_ref[src * per + unit]), :] = acc[unit * UNIT:(unit + 1) * UNIT, :].astype(BF16)

        return carry

    lax.fori_loop(0, n_items, gather, 0)

    def store(slot):
        return pltpu.make_async_copy(obuf.at[slot], trash.at[slot], osem.at[slot])

    def expert(exp, done):
        slot = exp % 2
        for copy in weights(exp, slot):
            copy.wait()

        @pl.when(exp + 1 < local)
        def _():
            for copy in weights(exp + 1, 1 - slot):
                copy.start()

        begin, end = first_ref[exp], first_ref[exp + 1]

        def one_tile(index, done):
            unit0 = begin + index * tile_units
            x_val = rows_ref[pl.ds(pl.multiple_of(unit0 * UNIT, UNIT), tile), :]
            hid = dot(x_val, wgu[slot])
            gate = hid[:, :ff]
            act = (gate * jax.nn.sigmoid(gate) * hid[:, ff:]).astype(BF16)
            side = done % 2

            @pl.when(done >= 2)
            def _():
                store(side).wait()

            obuf[side] = dot(act, wdn[slot]).astype(BF16)
            for unit in range(tile_units):
                src = obuf.at[side, pl.ds(unit * UNIT, UNIT), :]

                @pl.when(unit0 + unit < end)
                def _():
                    pltpu.make_async_copy(src, out_hbm.at[unit_rows(inv_ref[jnp.minimum(unit0 + unit, n_src * per - 1)])], osem.at[side]).start()

                @pl.when(unit0 + unit >= end)
                def _():
                    pltpu.make_async_copy(src, trash.at[side, pl.ds(unit * UNIT, UNIT), :], osem.at[side]).start()

            return done + 1

        return lax.fori_loop(0, (end - begin + tile_units - 1) // tile_units, one_tile, done)

    n_exp = jnp.where(n_items > 0, local, 0)
    done = lax.fori_loop(0, n_exp, expert, 0)

    def drain(side):
        @pl.when(done > side)
        def _():
            store(side).wait()

    drain(0)
    drain(1)

    def blank_wait(index, carry):
        pltpu.make_async_copy(zbuf, out_hbm.at[pl.ds(0, UNIT), :], zsem).wait()
        return carry

    lax.fori_loop(used, n_src * per, blank_wait, 0)


def experts(index, tables, slots, gathered, w_gate, w_up, w_down):
    pos, inv, first, items, n_items = tables
    group, local, tokens = slots.shape
    n_req = len(gathered)
    _, width, ff = w_gate.shape
    tile = 256
    rows = group * PIECE
    info = jnp.stack([n_items[index], jnp.int32(index * PIECE)])
    kernel = functools.partial(expert_kernel, group, n_req=n_req, piece=PIECE)
    out, _ = pl.pallas_call(
        kernel,
        grid_spec=pltpu.PrefetchScalarGridSpec(
            num_scalar_prefetch=5,
            grid=(1,),
            in_specs=[whole_spec((group * local, tokens))] + [pl.BlockSpec(memory_space=ANY)] * (n_req + 3),
            out_specs=[pl.BlockSpec(memory_space=ANY)] * 2,
            scratch_shapes=[
                VMEM((2, width, 2 * ff), BF16),
                VMEM((2, ff, width), BF16),
                VMEM((rows + tile, width), BF16),
                VMEM((PIECE, width), F32),
                VMEM((3, KBLK, width), BF16),
                VMEM((2, tile, width), BF16),
                VMEM((UNIT, width), BF16),
                pltpu.SemaphoreType.DMA((2, 3)),
                pltpu.SemaphoreType.DMA((3,)),
                pltpu.SemaphoreType.DMA((2,)),
                pltpu.SemaphoreType.DMA,
            ],
        ),
        out_shape=[jax.ShapeDtypeStruct((rows, width), BF16), jax.ShapeDtypeStruct((2, tile, width), BF16)],
        compiler_params=pltpu.CompilerParams(vmem_limit_bytes=62 << 20),
        cost_estimate=pl.CostEstimate(flops=6 * rows * width * ff, bytes_accessed=6 * local * width * ff, transcendentals=rows * ff),
        name=f"experts_{index}",
    )(pos[index], inv[index], first[index], items[index], info, slots.reshape(group * local, tokens), *gathered, w_gate, w_up, w_down)
    return out.reshape(group, PIECE, width)


def sum_kernel(item_ref, count_ref, len_ref, slot_ref, prob_ref, back_ref, *refs, n_req, piece):
    accs = refs[n_req + 1:2 * n_req + 1]
    y_hbm, gates, abuf, ybuf, isem, osem, ysem = refs[2 * n_req + 1:]
    group = back_ref.shape[0] // piece
    local = slot_ref.shape[0] // group
    base = count_ref[1]
    n_items = count_ref[0]
    req_blk = slot_ref.shape[1] // TBLK // n_req
    chunk = req_blk * TBLK

    def each(blk, todo):
        for req in range(n_req):
            @pl.when(blk // req_blk == req)
            def _():
                todo(accs[req].at[pl.ds(pl.multiple_of((blk % req_blk) * TBLK, TBLK), TBLK), :])

    def load(index):
        side = index % 2
        each(item_ref[index], lambda ref: pltpu.make_async_copy(ref, abuf.at[side], isem.at[side]).start())

    def save_wait(side):
        pltpu.make_async_copy(abuf.at[side], accs[0].at[pl.ds(0, TBLK), :], osem.at[side]).wait()
        pltpu.make_async_copy(ybuf.at[side], y_hbm.at[pl.ds(0, TBLK), :], ysem.at[side]).wait()

    @pl.when(n_items > 0)
    def _():
        load(0)

    def body(index, carry):
        blk = item_ref[index]
        side = index % 2
        cols = pl.ds(pl.multiple_of(blk * TBLK, TBLK), TBLK)
        row = lax.broadcasted_iota(jnp.int32, (piece, TBLK), 0)
        for owner in range(group):
            at = slot_ref[owner * local:(owner + 1) * local, cols] - base
            prob = prob_ref[owner * local:(owner + 1) * local, cols]
            gate = jnp.zeros((piece, TBLK), F32)
            for exp in range(local):
                gate = jnp.where(at[exp:exp + 1, :] == row, prob[exp:exp + 1, :], gate)
            high = gate.astype(BF16)
            rest = gate - high.astype(F32)
            mid = rest.astype(BF16)
            low = (rest - mid.astype(F32)).astype(BF16)
            rows = slice(owner * piece, (owner + 1) * piece)
            gates[rows, 0:TBLK] = high
            gates[rows, TBLK:2 * TBLK] = mid
            gates[rows, 2 * TBLK:3 * TBLK] = low
        pltpu.make_async_copy(accs[0].at[pl.ds(0, TBLK), :], abuf.at[side], isem.at[side]).wait()

        @pl.when(index >= 1)
        def _():
            save_wait(1 - side)

        @pl.when(index + 1 < n_items)
        def _():
            load(index + 1)

        req = blk // req_blk
        keep = len_ref[req] - (blk % req_blk) * TBLK
        good = lax.broadcasted_iota(jnp.int32, (TBLK, 1), 0) < keep
        width = abuf.shape[2]
        step = 512

        def column(part, carry):
            at = pl.ds(pl.multiple_of(part * step, step), step)
            out = lax.dot_general(gates[...], back_ref[:, at], (((0,), (0,)), ((), ())), preferred_element_type=F32)
            total = abuf[side, :, at] + (out[0:TBLK] + (out[TBLK:2 * TBLK] + out[2 * TBLK:]))
            abuf[side, :, at] = total
            ybuf[side, :, at] = jnp.where(good, total, 0.0).astype(BF16)
            return carry

        lax.fori_loop(0, width // step, column, 0)
        each(blk, lambda ref: pltpu.make_async_copy(abuf.at[side], ref, osem.at[side]).start())
        pltpu.make_async_copy(ybuf.at[side], y_hbm.at[cols, :], ysem.at[side]).start()
        return carry

    lax.fori_loop(0, n_items, body, 0)

    @pl.when(n_items > 0)
    def _():
        save_wait((n_items - 1) % 2)


def sum_piece(index, home, lens, slot, prob, back, accs, y_buf):
    items, n_items = home
    n_exp, tokens = slot.shape
    group, piece, width = back.shape
    n_req = len(accs)
    info = jnp.stack([n_items[index], jnp.int32(index * PIECE)])
    outs = pl.pallas_call(
        functools.partial(sum_kernel, n_req=n_req, piece=piece),
        grid_spec=pltpu.PrefetchScalarGridSpec(
            num_scalar_prefetch=3,
            grid=(1,),
            in_specs=[whole_spec((n_exp, tokens)), whole_spec((n_exp, tokens)), whole_spec((group * piece, width))] + [pl.BlockSpec(memory_space=ANY)] * (n_req + 1),
            out_specs=[pl.BlockSpec(memory_space=ANY)] * (n_req + 1),
            scratch_shapes=[
                VMEM((group * piece, 3 * TBLK), BF16),
                VMEM((2, TBLK, width), F32),
                VMEM((2, TBLK, width), BF16),
                pltpu.SemaphoreType.DMA((2,)),
                pltpu.SemaphoreType.DMA((2,)),
                pltpu.SemaphoreType.DMA((2,)),
            ],
        ),
        out_shape=[jax.ShapeDtypeStruct(acc.shape, F32) for acc in accs] + [jax.ShapeDtypeStruct(y_buf.shape, BF16)],
        input_output_aliases={6 + i: i for i in range(n_req + 1)},
        compiler_params=pltpu.CompilerParams(vmem_limit_bytes=40 << 20),
        cost_estimate=pl.CostEstimate(flops=2 * 3 * 512 * group * piece * width, bytes_accessed=16 << 20, transcendentals=0),
        name=f"sum_{index}",
    )(items[index], info, lens, slot, prob, back.reshape(group * piece, width), *accs, y_buf)
    return outs[:n_req], outs[n_req]


def solution(mesh):
    group = mesh.shape['dpa']
    tok_spec = P(('dp', 'dpa'))
    whole = P()
    exp_spec = P('dpa')

    def device_step(x_in, chunk_len, ctx_len, lat_cache, rope_cache, topk_idx, g_attn, w_q, w_dkv, g_kv, w_kr, w_uk, w_uv, w_o, g_ffn, w_router, w_sh_gate, w_sh_up, w_sh_down, w_exp_gate, w_exp_up, w_exp_down):
        _, n_req, chunk, width = x_in.shape
        rope = w_kr.shape[1]
        half = rope // 2
        heads, vdim = w_o.shape[:2]
        tokens = n_req * chunk
        top_k = topk_idx.shape[-1]
        n_exp = w_router.shape[1]
        local = n_exp // group
        capacity = tokens * top_k // group
        cap_units = capacity // UNIT + local
        n_pieces = -(-cap_units * UNIT // PIECE)
        lens, ctx = chunk_len[0], ctx_len[0]
        x_all = x_in[0]

        valid = (jnp.arange(chunk)[None, :] < lens[:, None]).reshape(tokens)
        slot, n_units = slot_table(topk_idx.reshape(tokens, top_k), valid, n_exp, group)
        slots = lax.all_to_all(slot.reshape(group, local, tokens), 'dpa', 0, 0, tiled=True)
        tables = owner_tables(slots, n_pieces)
        own_piece = jnp.where(slot >= 0, slot // PIECE, -1).reshape(n_exp, tokens // TBLK, TBLK)
        home = compact(jnp.any(own_piece[None] == jnp.arange(n_pieces, dtype=jnp.int32)[:, None, None, None], axis=(1, 3)))

        inv_freq = THETA ** (-2.0 * jnp.arange(half, dtype=F32) / rope)
        angle = (ctx[:, None] + jnp.arange(chunk)).astype(F32)[..., None] * inv_freq
        cos_tab = jnp.concatenate([jnp.cos(angle), jnp.cos(angle)], axis=-1)
        sin_tab = jnp.concatenate([-jnp.sin(angle), jnp.sin(angle)], axis=-1)
        perm = jnp.roll(jnp.eye(rope, dtype=F32), half, axis=1).astype(BF16)
        wkr2 = jnp.concatenate([w_kr, w_kr[:, half:], w_kr[:, :half]], axis=1)
        wuk = w_uk.transpose(1, 2, 0)
        wuv = w_uv.transpose(1, 0, 2)
        wo = w_o.reshape(heads * vdim, width)
        lat_all, rope_all = lat_cache[0], rope_cache[0]
        gathered, accs, probs = [], [], []
        for req in range(n_req):
            a_req = rms_norm(x_all[req], g_attn)
            q_req = jnp.einsum('cd,dhq->hcq', a_req, w_q, preferred_element_type=F32).astype(BF16)
            h_req, u_req, lat_all, rope_all = attention(req, jnp.stack([lens[req], ctx[req]]), x_all, a_req, q_req, wuk, wuv, w_dkv, wkr2, cos_tab, sin_tab, perm, g_kv[None], g_ffn[None], wo, lat_all, rope_all)
            gathered.append(lax.all_gather(u_req, 'dpa', axis=0, tiled=True))
            probs.append(jax.nn.softmax(dot(u_req, w_router), axis=-1).T)
            act = (jax.nn.silu(dot(u_req, w_sh_gate)) * dot(u_req, w_sh_up)).astype(BF16)
            accs.append(h_req.astype(F32) + dot(act, w_sh_down))
        prob = jnp.concatenate(probs, axis=1)

        y_buf = jnp.zeros((tokens, width), BF16)
        for index in range(n_pieces):
            sent = experts(index, tables, slots, gathered, w_exp_gate, w_exp_up, w_exp_down)
            back = lax.all_to_all(sent, 'dpa', 0, 0, tiled=True)
            accs, y_buf = sum_piece(index, home, lens, slot, prob, back, accs, y_buf)
        return y_buf.reshape(x_in.shape), lat_all[None], rope_all[None]

    return jax.shard_map(device_step, mesh=mesh, in_specs=(tok_spec,) * 6 + (whole,) * 13 + (exp_spec,) * 3, out_specs=(tok_spec, tok_spec, tok_spec), check_vma=False)
```

```python
import functools

import jax
import jax.numpy as jnp
from jax import lax
from jax.experimental import pallas as pl
from jax.experimental.pallas import tpu as pltpu
from jax.sharding import PartitionSpec as P


EPS = 1e-6
THETA = 10000.0
NEG = -1e30
UNIT = 16
PIECE = 256
FIXED = 4
PART = 128
TBLK = 128
TERMS = 3
COLS = 512
GROUP_BLKS = 4
EARLY = 3
N = None
I32 = jnp.int32
FIRST_DIMS = (((0,), (0,)), ((), ()))
LAST_DIMS = (((1,), (1,)), ((), ()))
MIB = 1 << 20
VMEM = pltpu.VMEM
ANY = pl.ANY
F32 = jnp.float32
BF16 = jnp.bfloat16


def rms_norm(vals, gain):
    vals_f32 = vals.astype(F32)
    inv_rms = lax.rsqrt(jnp.mean(vals_f32 * vals_f32, axis=-1, keepdims=True) + EPS)
    return (vals_f32 * inv_rms * gain.astype(F32)).astype(BF16)


def dot(lhs, rhs):
    return jnp.dot(lhs, rhs, preferred_element_type=F32)


def whole_spec(shape):
    return pl.BlockSpec(shape, lambda *_: (0,) * len(shape), pipeline_mode=pl.Buffered(1))


def attention_kernel(info, x_hbm, a_ref, q_ref, wuk_ref, wuv_ref, wdkv_ref, wkr_ref, cos_ref, sin_ref, gkv_ref, gffn_ref, wo_hbm, lat_ref, rope_ref, h_ref, u_ref, lat_out, rope_out, keys_ref, o_ref, xbuf, wo_ref, sems, *, heads_step, row_blk, key_blk, scale, nope):
    step = pl.program_id(0)
    count, ctx, req = (info[i] for i in range(3))
    chunk, width = a_ref.shape
    rank = lat_ref.shape[1]
    ctx_max = lat_ref.shape[0]
    rope = rope_ref.shape[0]
    half = rope // 2
    late = (
        pltpu.make_async_copy(x_hbm.at[req], xbuf, sems.at[0]),
        pltpu.make_async_copy(wo_hbm, wo_ref, sems.at[1]),
    )

    def turned(vals, cols):
        other = jnp.concatenate([vals[half:], vals[:half]], axis=0)
        return (vals * cos_ref[:, cols] + other * sin_ref[:, cols]).astype(BF16)

    @pl.when(step == 0)
    def _():
        for copy in late:
            copy.start()
        a_val = a_ref[...]
        lat_f32 = dot(a_val, wdkv_ref[...])
        inv_rms = lax.rsqrt(jnp.mean(lat_f32 * lat_f32, axis=-1, keepdims=True) + EPS)
        lat_new = (lat_f32 * inv_rms * gkv_ref[...].astype(F32)).astype(BF16)
        rope_new = turned(dot(a_val, wkr_ref[...]).T, slice(None))
        for base in range(0, ctx_max, key_blk):
            rows = pl.ds(base, key_blk)
            touched = (base < ctx + count) & (base + key_blk > ctx)

            @pl.when(touched)
            def _():
                pos = lax.broadcasted_iota(I32, (key_blk, chunk), 0) + base - ctx
                row = lax.broadcasted_iota(I32, (key_blk, chunk), 1)
                pick = (pos == row).astype(F32).astype(BF16)
                at = lax.broadcasted_iota(I32, (key_blk, 1), 0) + base - ctx
                lat_blk = jnp.where((at >= 0) & (at < count), dot(pick, lat_new), lat_ref[rows, :].astype(F32))
                lat_out[rows, :] = lat_blk.astype(BF16)
                keys_ref[0:rank, rows] = lat_blk.T.astype(BF16)
                moved = lax.dot_general(rope_new, pick, LAST_DIMS, preferred_element_type=F32)
                at = lax.broadcasted_iota(I32, (1, key_blk), 1) + base - ctx
                rope_blk = jnp.where((at >= 0) & (at < count), moved, rope_ref[:, rows].astype(F32)).astype(BF16)
                rope_out[:, rows] = rope_blk
                keys_ref[rank:rank + rope, rows] = rope_blk

            @pl.when(jnp.logical_not(touched))
            def _():
                lat_out[rows, :] = lat_ref[rows, :]
                keys_ref[0:rank, rows] = lat_ref[rows, :].astype(F32).T.astype(BF16)
                rope_out[:, rows] = rope_ref[:, rows]
                keys_ref[rank:rank + rope, rows] = rope_ref[:, rows]

    vdim = wuv_ref.shape[2]
    n_rows = (count + row_blk - 1) // row_blk

    def row_block(index, carry):
        row0 = pl.multiple_of(index * row_blk, row_blk)
        rows = pl.ds(row0, row_blk)
        blocks = (ctx + jnp.minimum(count, row0 + row_blk) + key_blk - 1) // key_blk

        def variant(n_keys):
            span = n_keys * key_blk
            col = lax.broadcasted_iota(I32, (row_blk, span), 1)
            row = lax.broadcasted_iota(I32, (row_blk, span), 0)
            visible = col - row <= ctx + row0
            q_lat, q_rot, probs = {}, {}, {}

            def query(sub):
                q_lat[sub] = lax.dot_general(q_ref[sub, 0:nope, rows], wuk_ref[sub], FIRST_DIMS, preferred_element_type=F32).astype(BF16)
                q_rot[sub] = turned(q_ref[sub, nope:nope + rope, rows].astype(F32), rows)

            def score(sub):
                both = dot(q_lat[sub], keys_ref[0:rank, :span]) + lax.dot_general(q_rot[sub], keys_ref[rank:rank + rope, :span], FIRST_DIMS, preferred_element_type=F32)
                probs[sub] = jnp.where(visible, both * scale, NEG)

            def soften(sub):
                expo = jnp.exp(probs[sub] - jnp.max(probs[sub], axis=1, keepdims=True))
                probs[sub] = (expo * (1.0 / jnp.sum(expo, axis=1, keepdims=True))).astype(BF16)

            def finish(sub):
                out_lat = dot(probs[sub], lat_out[0:span, :]).astype(BF16)
                head = step * heads_step + sub
                o_ref[rows, pl.ds(pl.multiple_of(head * vdim, vdim), vdim)] = dot(out_lat, wuv_ref[sub]).astype(BF16)

            for sub in range(heads_step):
                query(sub)
            score(0)
            for sub in range(heads_step):
                if sub + 1 < heads_step:
                    score(sub + 1)
                soften(sub)
                finish(sub)

        most = ctx_max // key_blk
        for n_keys in range(2, most + 1):
            @pl.when((blocks == n_keys) | ((n_keys == 2) & (blocks < 2)))
            def _():
                variant(n_keys)

        return carry

    lax.fori_loop(0, n_rows, row_block, 0)

    @pl.when(step == pl.num_programs(0) - 1)
    def _():
        for copy in late:
            copy.wait()

        def project(index, carry):
            rows = pl.ds(pl.multiple_of(index * row_blk, row_blk), row_blk)

            def column(part, carry):
                cols = pl.ds(pl.multiple_of(part * 512, 512), 512)
                attn = dot(o_ref[rows, :], wo_ref[:, cols]).astype(BF16)
                h_ref[rows, cols] = (xbuf[rows, cols].astype(F32) + attn.astype(F32)).astype(BF16)
                return carry

            lax.fori_loop(0, width // 512, column, 0)
            u_ref[rows, :] = rms_norm(h_ref[rows, :], gffn_ref[...])
            return carry

        def blank(index, carry):
            rows = pl.ds(pl.multiple_of(index * row_blk, row_blk), row_blk)
            h_ref[rows, :] = jnp.zeros((row_blk, width), BF16)
            u_ref[rows, :] = jnp.zeros((row_blk, width), BF16)
            return carry

        lax.fori_loop(0, n_rows, project, 0)
        lax.fori_loop(n_rows, chunk // row_blk, blank, 0)


def attention(info, x_all, a_req, q_req, wuk, wuv, wdkv, wkr, cos_tab, sin_tab, gkv, gffn, wo, lat_all, rope_all):
    _, chunk, width = x_all.shape
    heads, qdim, _ = q_req.shape
    rope = wkr.shape[1]
    nope = qdim - rope
    _, ctx_max, rank = lat_all.shape
    vdim = wuv.shape[2]
    hstep = 4
    kernel = functools.partial(attention_kernel, heads_step=hstep, row_blk=256, key_blk=256, scale=qdim ** -0.5, nope=nope)

    def one(shape):
        return pl.BlockSpec((N,) + shape, lambda _, info: (info[2],) + (0,) * len(shape), pipeline_mode=pl.Buffered(1))

    def per_head(shape):
        return pl.BlockSpec((hstep,) + shape, lambda i, *_: (i, 0, 0))

    return pl.pallas_call(
        kernel,
        grid_spec=pltpu.PrefetchScalarGridSpec(
            num_scalar_prefetch=1,
            grid=(heads // hstep,),
            in_specs=[
                pl.BlockSpec(memory_space=ANY),
                whole_spec((chunk, width)),
                per_head((qdim, chunk)),
                per_head((nope, rank)),
                per_head((rank, vdim)),
                whole_spec(wdkv.shape),
                whole_spec(wkr.shape),
                one((rope, chunk)),
                one((rope, chunk)),
                whole_spec(gkv.shape),
                whole_spec(gffn.shape),
                pl.BlockSpec(memory_space=ANY),
                one((ctx_max, rank)),
                one((rope, ctx_max)),
            ],
            out_specs=[
                whole_spec((chunk, width)),
                whole_spec((chunk, width)),
                one((ctx_max, rank)),
                one((rope, ctx_max)),
            ],
            scratch_shapes=[
                VMEM((rank + rope, ctx_max), BF16),
                VMEM((chunk, heads * vdim), BF16),
                VMEM((chunk, width), BF16),
                VMEM(wo.shape, BF16),
                pltpu.SemaphoreType.DMA((2,)),
            ],
        ),
        out_shape=[
            jax.ShapeDtypeStruct((chunk, width), BF16),
            jax.ShapeDtypeStruct((chunk, width), BF16),
            jax.ShapeDtypeStruct(lat_all.shape, BF16),
            jax.ShapeDtypeStruct(rope_all.shape, BF16),
        ],
        input_output_aliases={13: 2, 14: 3},
        compiler_params=pltpu.CompilerParams(vmem_limit_bytes=58 * MIB),
        cost_estimate=pl.CostEstimate(flops=chunk * heads * ctx_max * rank * 4, bytes_accessed=24 * MIB, transcendentals=chunk * heads * ctx_max // 2),
    )(info, x_all, a_req, q_req, wuk, wuv, wdkv, wkr, cos_tab, sin_tab, gkv, gffn, wo, lat_all, rope_all)


def shared_kernel(lens, u_ref, h_ref, wr_ref, wg_hbm, wu_hbm, wd_hbm, total_ref, prob_ref, wg, wu, wd, act, sems):
    index = pl.program_id(0)
    blk, width = u_ref.shape
    ff = act.shape[1]
    step = ff // 2
    copies = [pltpu.make_async_copy(*pair, sems.at[i]) for i, pair in enumerate(((wg_hbm, wg), (wu_hbm, wu), (wd_hbm, wd)))]

    @pl.when(index == 0)
    def _():
        for copy in copies:
            copy.start()

    def wait(some):
        @pl.when(index == 0)
        def _():
            for copy in some:
                copy.wait()

    @pl.when((index * blk < lens[0]) | (index == 0))
    def _():
        logits = lax.dot_general(wr_ref[...], u_ref[...], LAST_DIMS, preferred_element_type=F32)
        expo = jnp.exp(logits - jnp.max(logits, axis=0, keepdims=True))
        prob_ref[...] = expo / jnp.sum(expo, axis=0, keepdims=True)
        wait(copies[:2])
        for part in range(2):
            cols = slice(part * step, (part + 1) * step)
            gate = dot(u_ref[...], wg[:, cols])
            act[:, cols] = (gate * jax.nn.sigmoid(gate) * dot(u_ref[...], wu[:, cols])).astype(BF16)
        wait(copies[2:])
        for start in range(0, width, COLS):
            cols = slice(start, start + COLS)
            total_ref[:, cols] = h_ref[:, cols].astype(F32) + dot(act[...], wd[:, cols])


def shared(count, u_req, h_req, w_router, w_gate, w_up, w_down):
    chunk, width = u_req.shape
    ff = w_gate.shape[1]
    n_exp = w_router.shape[1]
    blk = PIECE
    rows = pl.BlockSpec((blk, width), lambda i, *_: (i, 0))
    return pl.pallas_call(
        shared_kernel,
        grid_spec=pltpu.PrefetchScalarGridSpec(
            num_scalar_prefetch=1,
            grid=(chunk // blk,),
            in_specs=[rows, rows, whole_spec((n_exp, width))] + [pl.BlockSpec(memory_space=ANY)] * 3,
            out_specs=[rows, pl.BlockSpec((n_exp, blk), lambda i, *_: (0, i))],
            scratch_shapes=[VMEM(w_gate.shape, BF16), VMEM(w_up.shape, BF16), VMEM(w_down.shape, BF16), VMEM((blk, ff), BF16), pltpu.SemaphoreType.DMA((3,))],
        ),
        out_shape=[jax.ShapeDtypeStruct((chunk, width), F32), jax.ShapeDtypeStruct((n_exp, chunk), F32)],
        compiler_params=pltpu.CompilerParams(vmem_limit_bytes=62 * MIB),
        cost_estimate=pl.CostEstimate(flops=6 * chunk * width * ff, bytes_accessed=6 * width * ff, transcendentals=chunk * ff),
    )(count, u_req, h_req, w_router.T, w_gate, w_up, w_down)


def unit_ranks(units, turn):
    local = units.shape[-1]
    own = jnp.arange(local, dtype=I32)[:, N]
    rank = jnp.zeros_like(turn)
    for other in range(local):
        have = units[..., other][..., None, None]
        rank = rank + jnp.minimum(have, turn) + ((own > other) & (have > turn)).astype(I32)
    return rank


def slot_table(topk, valid, n_exp, group):
    tokens = topk.shape[0]
    local = n_exp // group
    ids = jnp.arange(n_exp, dtype=I32)
    hit = jnp.any(topk.T[:, None, :] == ids[None, :, None], axis=0) & valid[N, :]
    ones = hit.astype(BF16).reshape(n_exp, tokens // 128, 128)
    low = (jnp.arange(128)[:, N] < jnp.arange(128)[N, :]).astype(BF16)
    inner = jnp.einsum('ebt,ts->ebs', ones, low, preferred_element_type=F32)
    sums = jnp.sum(ones.astype(F32), axis=2)
    n_blk = tokens // 128
    outer = jnp.einsum('eb,bc->ec', sums.astype(BF16), (jnp.arange(n_blk)[:, N] < jnp.arange(n_blk)[N, :]).astype(BF16), preferred_element_type=F32)
    before = (inner + outer[:, :, None]).astype(I32).reshape(group, local, tokens)
    units = (jnp.sum(sums, axis=1).astype(I32).reshape(group, local) + UNIT - 1) // UNIT
    slot = unit_ranks(units, before // UNIT) * UNIT + before % UNIT
    return jnp.where(hit, slot.reshape(n_exp, tokens), -1), jnp.sum(units, axis=1)


def compact(active):
    size = active.shape[-1]
    ids = jnp.arange(size, dtype=I32)
    flag = active.astype(I32)
    place = jnp.sum(jnp.where(ids[N, :] < ids[:, N], flag[..., None, :], 0), axis=-1)
    items = jnp.sum(jnp.where((place[..., None, :] == ids[:, N]) & active[..., None, :], ids, 0), axis=-1)
    return items, jnp.sum(flag, axis=-1)


def piece_of(slot, starts):
    return sum((slot >= first).astype(I32) for first in starts) - 1


def owner_tables(slots, starts, sizes):
    group, local, tokens = slots.shape
    n_pieces = len(starts)
    per = max(sizes) // UNIT
    units = (jnp.sum((slots >= 0).astype(I32), axis=2) + UNIT - 1) // UNIT
    places = jnp.arange(per, dtype=I32)
    ranks = jnp.array(starts, I32)[:, N] // UNIT + places
    real = places < jnp.array(sizes, I32)[:, N] // UNIT
    flat = ranks.reshape(-1)
    turns = jnp.arange(tokens // UNIT + 1, dtype=I32)
    until = jnp.sum(jnp.minimum(units[:, :, N], turns), axis=1)
    turn = jnp.sum((until[:, N, 1:] <= flat[:, N]).astype(I32), axis=2)
    start = jnp.sum(jnp.minimum(units[:, N, :], turn[:, :, N]), axis=2)
    has = units[:, N, :] > turn[:, :, N]
    upto = jnp.sum((has[:, :, N, :] & (jnp.arange(local)[N, :] <= jnp.arange(local)[:, N])).astype(I32), axis=3)
    expert = jnp.sum((upto <= (flat - start)[:, :, N]).astype(I32), axis=2).reshape(group, n_pieces, per)
    expert = jnp.where(real, expert, local + 1).transpose(1, 0, 2).reshape(n_pieces, group * per)
    order = jnp.arange(group * per, dtype=I32)
    key = expert * (group * per) + order
    pos = jnp.sum((key[:, N, :] < key[:, :, N]).astype(I32), axis=2)
    inv = jnp.sum(jnp.where(pos[:, N, :] == order[:, N], order, 0), axis=2)
    first = jnp.sum((expert[:, N, :] < jnp.arange(local + 2, dtype=I32)[:, N]).astype(I32), axis=2)
    n_blk = tokens // TBLK
    piece = piece_of(slots, starts).reshape(group, local, n_blk, TBLK)
    active = jnp.any(piece == jnp.arange(n_pieces, dtype=I32)[:, N, N, N, N], axis=(2, 4))
    blocks, n_blocks = compact(active)
    groups = jnp.arange(n_blk // GROUP_BLKS, dtype=I32) * GROUP_BLKS
    items, n_items = compact((n_blocks[:, :, N] > groups).reshape(n_pieces, group * (n_blk // GROUP_BLKS)))
    return pos, inv, first, blocks.reshape(n_pieces, group * n_blk), n_blocks, items, n_items


def home_tables(slot, group, n_chunks, starts):
    n_exp, tokens = slot.shape
    local = n_exp // group
    n_blk = tokens // TBLK
    slot = slot.reshape(group, local, n_blk, TBLK)
    chunk = jnp.where(slot >= 0, slot // PART, -1)
    active = jnp.any(chunk == jnp.arange(n_chunks, dtype=I32)[:, N, N, N, N], axis=(2, 4))
    chunks, n_used = compact(active.transpose(2, 0, 1).reshape(n_blk, n_chunks * group))
    last = jnp.max(piece_of(slot, starts), axis=(0, 1, 3))
    blocks, n_ready = compact(last == jnp.arange(len(starts), dtype=I32)[:, N])
    return chunks, n_used, blocks, n_ready


def expert_kernel(pos_ref, inv_ref, first_ref, blk_ref, nblk_ref, item_ref, info_ref, slot_ref, *refs, n_req, n_out, n_slots, base, stride):
    u_refs = refs[:n_req]
    wg_hbm, wu_hbm, wd_hbm = refs[n_req:n_req + 3]
    outs = refs[n_req + 3:n_req + 3 + n_out]
    trash, wgu, wdn, rows_ref, acc, ubuf, obuf, zbuf, wsem, usem, osem, zsem = refs[n_req + 3 + n_out:]
    local, _, ff = wg_hbm.shape
    piece = acc.shape[0]
    per = piece // UNIT
    tile = obuf.shape[1]
    tile_units = tile // UNIT
    n_blk = slot_ref.shape[1] // TBLK
    n_grp = n_blk // GROUP_BLKS
    req_blk = n_blk // n_slots
    n_items = info_ref[0]

    def weights(exp, slot):
        return (
            pltpu.make_async_copy(wg_hbm.at[exp], wgu.at[slot, :, pl.ds(0, ff)], wsem.at[slot, 0]),
            pltpu.make_async_copy(wu_hbm.at[exp], wgu.at[slot, :, pl.ds(ff, ff)], wsem.at[slot, 1]),
            pltpu.make_async_copy(wd_hbm.at[exp], wdn.at[slot], wsem.at[slot, 2]),
        )

    def each_block(index, todo):
        item = item_ref[index]
        src, grp = item // n_grp, item % n_grp
        for part in range(GROUP_BLKS):
            place = grp * GROUP_BLKS + part

            @pl.when(place < nblk_ref[src])
            def _():
                todo(src, blk_ref[src * n_blk + place], part)

    def fetch(index):
        side = index % 2

        def one(src, blk, part):
            start = pl.multiple_of((src * req_blk + blk % req_blk) * TBLK, TBLK)
            for req in range(n_req):
                @pl.when(blk // req_blk == req)
                def _():
                    pltpu.make_async_copy(u_refs[req].at[pl.ds(start, TBLK), :], ubuf.at[side, pl.ds(part * TBLK, TBLK), :], usem.at[side]).start()

        each_block(index, one)

    def fetched(index):
        side = index % 2

        def one(src, blk, part):
            pltpu.make_async_copy(u_refs[0].at[pl.ds(0, TBLK), :], ubuf.at[side, pl.ds(part * TBLK, TBLK), :], usem.at[side]).wait()

        each_block(index, one)

    def unit_rows(unit):
        return pl.ds(pl.multiple_of(unit * UNIT, UNIT), UNIT)

    def send(src_ref, unit, sem):
        src, place = unit // stride, unit % stride
        each = per // n_out
        for part in range(n_out):
            @pl.when(place // each == part)
            def _():
                pltpu.make_async_copy(src_ref, outs[part].at[unit_rows(src * each + place % each)], sem).start()

    @pl.when(n_items > 0)
    def _():
        ubuf[...] = jnp.zeros_like(ubuf)
        fetch(0)
        for copy in weights(0, 0):
            copy.start()

    zbuf[...] = jnp.zeros_like(zbuf)
    used, whole = first_ref[local], first_ref[local + 1]

    def blank(index, carry):
        send(zbuf, inv_ref[index], zsem)
        return carry

    lax.fori_loop(used, whole, blank, 0)

    def gather(index, carry):
        item = item_ref[index]
        src, grp = item // n_grp, item % n_grp
        side = index % 2

        @pl.when(index + 1 < n_items)
        def _():
            fetch(index + 1)

        row = lax.broadcasted_iota(I32, (piece, TBLK), 0)
        picks = []
        for part in range(GROUP_BLKS):
            place = grp * GROUP_BLKS + part
            blk = blk_ref[src * n_blk + jnp.minimum(place, n_blk - 1)]
            at = slot_ref[pl.ds(pl.multiple_of(src * local, local), local), pl.ds(pl.multiple_of(blk * TBLK, TBLK), TBLK)] - base
            at = jnp.where(place < nblk_ref[src], at, -1)
            pick = jnp.zeros((piece, TBLK), F32)
            for exp in range(local):
                pick = jnp.where(at[exp:exp + 1, :] == row, 1.0, pick)
            picks.append(pick.astype(BF16))
        pick = jnp.concatenate(picks, axis=1)
        fetched(index)

        @pl.when(grp == 0)
        def _():
            acc[...] = dot(pick, ubuf[side])

        @pl.when(grp > 0)
        def _():
            acc[...] += dot(pick, ubuf[side])

        @pl.when((grp + 1) * GROUP_BLKS >= nblk_ref[src])
        def _():
            for unit in range(per):
                rows_ref[unit_rows(pos_ref[src * stride + unit]), :] = acc[unit * UNIT:(unit + 1) * UNIT, :].astype(BF16)

        return carry

    lax.fori_loop(0, n_items, gather, 0)

    def store(slot):
        return pltpu.make_async_copy(obuf.at[slot], trash.at[slot], osem.at[slot])

    def expert(exp, done):
        slot = exp % 2

        @pl.when(exp + 1 < local)
        def _():
            for copy in weights(exp + 1, 1 - slot):
                copy.start()

        for copy in weights(exp, slot):
            copy.wait()
        begin, end = first_ref[exp], first_ref[exp + 1]

        def one_tile(index, done):
            unit0 = begin + index * tile_units
            x_val = rows_ref[pl.ds(pl.multiple_of(unit0 * UNIT, UNIT), tile), :]
            hid = dot(x_val, wgu[slot])
            gate = hid[:, :ff]
            act = (gate * jax.nn.sigmoid(gate) * hid[:, ff:]).astype(BF16)
            side = done % 2

            @pl.when(done >= 2)
            def _():
                store(side).wait()

            obuf[side] = dot(act, wdn[slot]).astype(BF16)

            def out(unit, carry):
                src_ref = obuf.at[side, unit_rows(unit), :]

                @pl.when(unit0 + unit < end)
                def _():
                    send(src_ref, inv_ref[unit0 + unit], osem.at[side])

                @pl.when(unit0 + unit >= end)
                def _():
                    pltpu.make_async_copy(src_ref, trash.at[side, unit_rows(unit), :], osem.at[side]).start()

                return carry

            lax.fori_loop(0, tile_units, out, 0)
            return done + 1

        return lax.fori_loop(0, (end - begin + tile_units - 1) // tile_units, one_tile, done)

    done = lax.fori_loop(0, jnp.where(n_items > 0, local, 0), expert, 0)
    for side in range(2):
        @pl.when(done > side)
        def _():
            store(side).wait()

    def blank_wait(index, carry):
        pltpu.make_async_copy(zbuf, outs[0].at[pl.ds(0, UNIT), :], zsem).wait()
        return carry

    lax.fori_loop(used, whole, blank_wait, 0)


def experts(index, tables, slots, gathered, w_gate, w_up, w_down, start, size, n_out):
    pos, inv, first, blocks, n_blocks, items, n_items = tables
    group, local, tokens = slots.shape
    n_req = len(gathered)
    _, width, ff = w_gate.shape
    tile = PIECE
    rows = group * size
    kernel = functools.partial(expert_kernel, n_req=n_req, n_out=n_out, n_slots=tokens * group // gathered[0].shape[0], base=start, stride=pos.shape[1] // group)
    outs = pl.pallas_call(
        kernel,
        grid_spec=pltpu.PrefetchScalarGridSpec(
            num_scalar_prefetch=7,
            grid=(1,),
            in_specs=[whole_spec((group * local, tokens))] + [pl.BlockSpec(memory_space=ANY)] * (n_req + 3),
            out_specs=[pl.BlockSpec(memory_space=ANY)] * (n_out + 1),
            scratch_shapes=[
                VMEM((2, width, 2 * ff), BF16),
                VMEM((2, ff, width), BF16),
                VMEM((rows + tile, width), BF16),
                VMEM((size, width), F32),
                VMEM((2, GROUP_BLKS * TBLK, width), BF16),
                VMEM((2, tile, width), BF16),
                VMEM((UNIT, width), BF16),
                pltpu.SemaphoreType.DMA((2, 3)),
                pltpu.SemaphoreType.DMA((2,)),
                pltpu.SemaphoreType.DMA((2,)),
                pltpu.SemaphoreType.DMA,
            ],
        ),
        out_shape=[jax.ShapeDtypeStruct((rows // n_out, width), BF16)] * n_out + [jax.ShapeDtypeStruct((2, tile, width), BF16)],
        compiler_params=pltpu.CompilerParams(vmem_limit_bytes=62 * MIB),
        cost_estimate=pl.CostEstimate(flops=6 * rows * width * ff, bytes_accessed=6 * local * width * ff, transcendentals=rows * ff),
    )(pos[index], inv[index], first[index], blocks[index], n_blocks[index], items[index], n_items[index:index + 1], slots.reshape(group * local, tokens), *gathered, w_gate, w_up, w_down)
    return [out.reshape(group, size // n_out, width) for out in outs[:n_out]]


def sum_kernel(blk_ref, nblk_ref, used_ref, chunk_ref, len_ref, turn_ref, slot_ref, prob_ref, *refs, n_req, n_back, n_chunks):
    totals, backs = refs[:n_req], refs[n_req:n_req + n_back]
    y_hbm, gates, rbuf, tbuf, acc, ybuf, todo_ref, rsem, tsem, ysem = refs[n_req + n_back + 1:]
    depth = rbuf.shape[0]
    n_exp = slot_ref.shape[0]
    width = tbuf.shape[2]
    n_blk = slot_ref.shape[1] // TBLK
    req_blk = n_blk // n_req
    group = backs[0].shape[0]
    local = n_exp // group
    n_ready = nblk_ref[0]
    per_blk = group * n_chunks

    def each_chunk(blk, grp, todo):
        for part in range(GROUP_BLKS):
            place = grp * GROUP_BLKS + part

            @pl.when(place < used_ref[blk])
            def _():
                item = chunk_ref[blk * per_blk + place]
                todo(item // group, item % group, part)

    def fetch(blk, grp, side):
        def one(chunk, owner, part):
            first = 0
            for ref in backs:
                have = ref.shape[1] // PART
                lo = first

                @pl.when((chunk >= lo) & (chunk < lo + have))
                def _():
                    start = pl.multiple_of((chunk - lo) * PART, PART)
                    pltpu.make_async_copy(ref.at[owner, pl.ds(start, PART), :], rbuf.at[side, pl.ds(part * PART, PART), :], rsem.at[side]).start()

                first += have

        each_chunk(blk, grp, one)

    def fetched(blk, grp, side):
        each_chunk(blk, grp, lambda chunk, owner, part: pltpu.make_async_copy(backs[0].at[0, pl.ds(0, PART), :], rbuf.at[side, pl.ds(part * PART, PART), :], rsem.at[side]).wait())

    def total_start(blk, side):
        rows = pl.ds(pl.multiple_of(blk % req_blk * TBLK, TBLK), TBLK)
        for req in range(n_req):
            @pl.when(blk // req_blk == req)
            def _():
                pltpu.make_async_copy(totals[req].at[rows, :], tbuf.at[side], tsem.at[side]).start()

    def y_copy(blk, side):
        start = (turn_ref[blk // req_blk] * req_blk + blk % req_blk) * TBLK
        return pltpu.make_async_copy(ybuf.at[side], y_hbm.at[pl.ds(pl.multiple_of(start, TBLK), TBLK), :], ysem.at[side])

    def at_item(index):
        item = todo_ref[index]
        return item // per_blk, item % per_blk

    def prefetch(index):
        @pl.when(index < n_items)
        def _():
            place, grp = at_item(index)
            fetch(blk_ref[place], grp, index % depth)

    def groups(index):
        return (used_ref[blk_ref[index]] + GROUP_BLKS - 1) // GROUP_BLKS

    def list_block(index, count):
        def one(grp, count):
            todo_ref[count] = index * per_blk + grp
            return count + 1

        return lax.fori_loop(0, groups(index), one, count)

    n_items = lax.fori_loop(0, n_ready, list_block, 0)

    @pl.when(n_ready > 0)
    def _():
        total_start(blk_ref[0], 0)
        rbuf[...] = jnp.zeros_like(rbuf)
        for index in range(depth - 1):
            prefetch(index)

    def step(index, carry):
        order, grp = at_item(index)
        blk = blk_ref[order]
        side = order % 2
        hand = index % depth
        cols = pl.ds(pl.multiple_of(blk * TBLK, TBLK), TBLK)
        prefetch(index + depth - 1)

        @pl.when(grp == 0)
        def _():
            pltpu.make_async_copy(totals[0].at[pl.ds(0, TBLK), :], tbuf.at[side], tsem.at[side]).wait()

            @pl.when(order + 1 < n_ready)
            def _():
                total_start(blk_ref[order + 1], 1 - side)

            acc[...] = tbuf[side]

        row = lax.broadcasted_iota(I32, (PART, TBLK), 0)
        for part in range(GROUP_BLKS):
            place = grp * GROUP_BLKS + part
            item = chunk_ref[blk * per_blk + jnp.minimum(place, per_blk - 1)]
            chunk, owner = item // group, item % group
            own = pl.ds(pl.multiple_of(owner * local, local), local)
            at = jnp.where(place < used_ref[blk], slot_ref[own, cols] - chunk * PART, -1)
            prob = prob_ref[own, cols]
            gate = jnp.zeros((PART, TBLK), F32)
            for exp in range(local):
                gate = jnp.where(at[exp:exp + 1, :] == row, prob[exp:exp + 1, :], gate)
            rows = slice(part * PART, (part + 1) * PART)
            for term in range(TERMS):
                high = gate.astype(BF16)
                gates[rows, term * TBLK:(term + 1) * TBLK] = high
                gate = gate - high.astype(F32)
        fetched(blk, grp, hand)
        for start in range(0, width, COLS):
            at = slice(start, start + COLS)
            out = lax.dot_general(gates[...], rbuf[hand, :, at], FIRST_DIMS, preferred_element_type=F32)
            acc[:, at] += sum(out[term * TBLK:(term + 1) * TBLK] for term in range(TERMS))

        @pl.when(grp + 1 == groups(order))
        def _():
            @pl.when(order >= 2)
            def _():
                y_copy(blk, side).wait()

            keep = len_ref[blk // req_blk] - (blk % req_blk) * TBLK
            good = lax.broadcasted_iota(I32, (TBLK, 1), 0) < keep
            ybuf[side] = jnp.where(good, acc[...], 0.0).astype(BF16)
            y_copy(blk, side).start()

        return carry

    lax.fori_loop(0, n_items, step, 0)
    for back in range(1, 3):
        @pl.when(n_ready >= back)
        def _():
            y_copy(0, (n_ready - back) % 2).wait()


def sum_ready(index, home, lens, turn, slot, prob, totals, backs, y_buf):
    chunks, n_used, blocks, n_ready = home
    n_exp, tokens = slot.shape
    group, _, width = backs[0].shape
    n_back, n_req = len(backs), len(totals)
    n_chunks = chunks.shape[1] // group
    (y_buf,) = pl.pallas_call(
        functools.partial(sum_kernel, n_req=n_req, n_back=n_back, n_chunks=n_chunks),
        grid_spec=pltpu.PrefetchScalarGridSpec(
            num_scalar_prefetch=6,
            grid=(1,),
            in_specs=[whole_spec((n_exp, tokens)), whole_spec((n_exp, tokens))] + [pl.BlockSpec(memory_space=ANY)] * (n_req + n_back + 1),
            out_specs=[pl.BlockSpec(memory_space=ANY)],
            scratch_shapes=[
                VMEM((GROUP_BLKS * PART, TERMS * TBLK), BF16),
                VMEM((3, GROUP_BLKS * PART, width), BF16),
                VMEM((2, TBLK, width), F32),
                VMEM((TBLK, width), F32),
                VMEM((2, TBLK, width), BF16),
                pltpu.SMEM((chunks.size // GROUP_BLKS + tokens // TBLK,), I32),
                pltpu.SemaphoreType.DMA((3,)),
                pltpu.SemaphoreType.DMA((2,)),
                pltpu.SemaphoreType.DMA((2,)),
            ],
        ),
        out_shape=[jax.ShapeDtypeStruct(y_buf.shape, BF16)],
        input_output_aliases={8 + n_req + n_back: 0},
        compiler_params=pltpu.CompilerParams(vmem_limit_bytes=40 * MIB),
        cost_estimate=pl.CostEstimate(flops=tokens * tokens * width, bytes_accessed=16 * MIB, transcendentals=0),
    )(blocks[index], n_ready[index:index + 1], n_used, chunks.reshape(-1), lens, turn, slot, prob, *totals, *backs, y_buf)
    return y_buf


def solution(mesh):
    group = mesh.shape['dpa']
    tok_spec = P(('dp', 'dpa'))
    whole = P()
    exp_spec = P('dpa')

    def after(value, *others):
        return lax.optimization_barrier((value,) + others)[0]

    def device_step(x_in, chunk_len, ctx_len, lat_cache, rope_cache, topk_idx, g_attn, w_q, w_dkv, g_kv, w_kr, w_uk, w_uv, w_o, g_ffn, w_router, w_sh_gate, w_sh_up, w_sh_down, w_exp_gate, w_exp_up, w_exp_down):
        _, n_req, chunk, width = x_in.shape
        rope = w_kr.shape[1]
        half = rope // 2
        heads, vdim = w_o.shape[:2]
        tokens = n_req * chunk
        top_k = topk_idx.shape[-1]
        n_exp = w_router.shape[1]
        local = n_exp // group
        capacity = tokens * top_k // group
        cap_rows = (capacity // UNIT + local) * UNIT
        starts = [index * PIECE for index in range(FIXED)] + [FIXED * PIECE]
        tail_parts = max(-(-(cap_rows - FIXED * PIECE) // PART), 1)
        near = (tail_parts + 1) // 2
        starts.append((FIXED + 0) * PIECE + near * PART)
        sizes = [PIECE] * FIXED + [near * PART, (tail_parts - near) * PART]
        lens, ctx = chunk_len[0], ctx_len[0]
        x_all = x_in[0]

        ids = jnp.arange(n_req, dtype=I32)
        ahead = (lens < lens[:, N]) | ((lens == lens[:, N]) & (ids < ids[:, N]))
        chosen = jnp.sum(ahead.astype(I32), axis=1) == ids[:, N]
        turn, lens_t, ctx_t = (jnp.sum(jnp.where(chosen, vals, 0), axis=1) for vals in (ids, lens, ctx))

        inv_freq = THETA ** (-2.0 * jnp.arange(half, dtype=F32) / rope)
        angle = inv_freq[:, N] * (ctx[:, N] + jnp.arange(chunk)).astype(F32)[:, N, :]
        cos_tab = jnp.concatenate([jnp.cos(angle), jnp.cos(angle)], axis=1)
        sin_tab = jnp.concatenate([-jnp.sin(angle), jnp.sin(angle)], axis=1)
        wuk = w_uk.transpose(1, 2, 0)
        wuv = w_uv.transpose(1, 0, 2)
        wo = w_o.reshape(heads * vdim, width)
        lat_all, rope_all = lat_cache[0], rope_cache[0].transpose(0, 2, 1)
        gathered, us, hs = [], [], []
        for index in range(n_req):
            x_req = lax.dynamic_index_in_dim(x_all, turn[index], keepdims=False)
            if us:
                x_req = after(x_req, us[-1])
            a_req = rms_norm(x_req, g_attn)
            q_req = jnp.einsum('cd,dhq->hqc', a_req, w_q, preferred_element_type=F32).astype(BF16)
            info = jnp.stack([lens_t[index], ctx_t[index], turn[index]])
            h_req, u_req, lat_all, rope_all = attention(info, x_all, a_req, q_req, wuk, wuv, w_dkv, w_kr, cos_tab, sin_tab, g_kv[N], g_ffn[N], wo, lat_all, rope_all)
            gathered.append(lax.all_gather(u_req, 'dpa', axis=0, tiled=True))
            us.append(u_req)
            hs.append(h_req)

        topk = after(topk_idx[0], us[0])
        topk = jnp.sum(jnp.where(chosen[:, :, N, N], topk, 0), axis=1).reshape(tokens, top_k)
        valid = (jnp.arange(chunk) < lens_t[:, N]).reshape(tokens)
        slot, n_units = slot_table(topk, valid, n_exp, group)
        slots = lax.all_to_all(slot.reshape(group, local, tokens), 'dpa', 0, 0, tiled=True)
        most = lax.pmax(jnp.max(n_units), 'dpa') * UNIT
        tables = owner_tables(slots, starts, sizes)
        head = min(EARLY, n_req)
        late_rows = slots[:, :, head * chunk:]
        early = jnp.logical_not(jnp.any((late_rows >= 0) & (late_rows < PIECE)))
        start = after(tables[0], most)

        def run(index, start, feeds, n_out):
            return experts(index, (start,) + tables[1:], slots, feeds, w_exp_gate, w_exp_up, w_exp_down, starts[index], sizes[index], n_out)

        first = lax.cond(early, lambda: run(0, start, gathered[:head], 1)[0], lambda: jnp.zeros((group, PIECE, width), BF16))
        first = lax.cond(early, lambda rows: rows, lambda rows: run(0, start, gathered, 1)[0], first)
        backs, totals, probs = [], [], []

        def share(req, mark):
            total, prob = shared(after(lens_t, mark)[req:req + 1], us[req], hs[req], w_router, w_sh_gate, w_sh_up, w_sh_down)
            totals.append(total)
            probs.append(prob)
            return prob

        mark = first
        for index in range(FIXED):
            sent = first
            if index:
                sent = run(index, after(tables[0], mark), gathered, 1)[0]
                mark = sent
                if index <= n_req:
                    mark = share(index - 1, sent)
                    sent = after(sent, mark)
            backs.append(lax.all_to_all(sent, 'dpa', 0, 0, tiled=True))
        home = home_tables(slot, group, sum(sizes) // PART, starts[:-1])
        start = after(tables[0], mark)
        tail = run(FIXED, start, gathered, near)
        mark = tail[0]
        for req in range(len(totals), n_req):
            mark = share(req, mark)
        prob = jnp.concatenate(probs, axis=1)
        y_buf = jnp.zeros((tokens, width), BF16)

        def add(index, backs, y_buf):
            return sum_ready(index, home, lens_t, turn, slot, prob, totals, backs, y_buf)

        for index in range(FIXED - 2):
            y_buf = add(index, backs[:index + 1], y_buf)

        def send(rows):
            return lax.all_to_all(rows, 'dpa', 0, 0, tiled=True)

        fixed = list(backs)
        for index in range(near):
            done = FIXED - 2 + index
            rows = after(tail[index], backs[-1], y_buf)
            if done < FIXED:
                def sums(y):
                    return add(done, fixed[:done + 1], y)

                extra, y_buf = lax.cond(most > FIXED * PIECE + index * PART, lambda rows, y: (send(rows), sums(y)), lambda rows, y: (rows, sums(y)), rows, y_buf)
            else:
                extra = lax.cond(most > FIXED * PIECE + index * PART, send, lambda rows: rows, rows)
            backs.append(extra)
        if sizes[-1]:
            backs.append(lax.cond(
                most > starts[-1],
                lambda start: send(run(FIXED + 1, start, gathered, 1)[0]),
                lambda start: jnp.zeros((group, sizes[-1], width), BF16),
                after(start, backs[-1])))
        y_buf = add(FIXED, backs, y_buf)
        return y_buf.reshape(x_in.shape), lat_all[N], rope_all.transpose(0, 2, 1)[N]

    return jax.shard_map(device_step, mesh=mesh, in_specs=(tok_spec,) * 6 + (whole,) * 13 + (exp_spec,) * 3, out_specs=(tok_spec, tok_spec, tok_spec), check_vma=False)
```
